256 devices in a mesh: dp: 64 (over z, y_lo, x), tensor: 4 (over y_hi, core).
Axes of the slice: x: 4, y: 4 (y_hi: 2, y_lo: 2; y = y_hi * 2 + y_lo), z: 8, core: 2. Of those that a mesh axis runs over, the one named last changes fastest.
Arguments:
- out_first: bfloat16 [64, 197, 1024], P('dp', None, 'tensor'), may hold values from -6 to 6
- out_second: bfloat16 [64, 197, 1024], P('dp', None, 'tensor'), may hold values from -6 to 6
- grad_first: bfloat16 [64, 197, 1024], P('dp', None, 'tensor'), may hold values from -6 to 6
- grad_second: bfloat16 [64, 197, 1024], P('dp', None, 'tensor'), may hold values from -16 to 16
- gain_attn: float32 [1024], replicated, may hold values from 0.25 to 1.75
- gain_mlp: float32 [1024], replicated, may hold values from 0.25 to 1.75
- qkv_weight: bfloat16 [1024, 3, 1024], P(None, None, 'tensor'), may hold values from -1 to 1
- proj_weight: bfloat16 [1024, 1024], P(None, 'tensor'), may hold values from -0.1875 to 0.1875
- inner_weight: bfloat16 [1024, 4096], P(None, 'tensor'), may hold values from -0.1875 to 0.1875
- inner_bias: float32 [4096], P('tensor'), may hold values from -3 to 3
- outer_weight: bfloat16 [1024, 4096], P(None, 'tensor'), may hold values from -0.09375 to 0.09375
Outputs:
- input_first: bfloat16 [64, 197, 1024], P('dp', None, 'tensor')
- input_second: bfloat16 [64, 197, 1024], P('dp', None, 'tensor')
- back_first: bfloat16 [64, 197, 1024], P('dp', None, 'tensor')
- back_second: bfloat16 [64, 197, 1024], P('dp', None, 'tensor')
- grad_qkv: float32 [1024, 3, 1024], P('dp', None, 'tensor')
- grad_proj: float32 [1024, 1024], P('dp', 'tensor')
- grad_inner: float32 [1024, 4096], P('dp', 'tensor')
- grad_bias: float32 [4096], P('tensor')
- grad_outer: float32 [1024, 4096], P('dp', 'tensor')
- grad_gain_attn: float32 [1024], P('tensor')
- grad_gain_mlp: float32 [1024], P('tensor')
The draws below stay inside these ranges and needn't reach their ends.
All inputs are finite; a program needn't handle non-finite values.
Results may differ from the reference program's by a relative error of at most 0.016.
Values may be sent and summed in bfloat16 or wider, within the bound.
No kernel may reach another device: no remote copies, remote signals or barrier semaphores. Data moves between devices by JAX's collectives and lax.ppermute only.
A program may use at most 64 MiB of HBM per device.

```python
import jax
import jax.numpy as jnp
from jax import lax

D = 1024
HEADS = 16
FF = 4096
SEQ = 197
IMAGES = 64


def draw_qkv_weight(key, part):
    base_key = jax.random.fold_in(key, 0)
    base_draw = jax.random.truncated_normal(base_key, -6.0, 6.0, (D, 3, D), jnp.float32) / D ** 0.5
    return jnp.clip(base_draw, -1.0, 1.0).astype(jnp.bfloat16)


def strengthened(array, own_key, source, target, blocks, factor):
    def block_of(axis_at):
        return (jnp.arange(array.shape[axis_at]) // (array.shape[axis_at] // blocks)).reshape((-1,) + (1,) * (array.ndim - 1 - axis_at))

    first = jax.random.permutation(own_key, blocks)[block_of(target)]
    other_side = (block_of(target) + blocks // 2) % blocks
    return jnp.where((block_of(source) == first) | (block_of(source) == other_side), factor * array, array)


def steps_of(key, shape, cuts, least, high):
    level = 1.0
    for axis_at, shards_of in cuts:
        heights = jax.random.uniform(jax.random.fold_in(jax.random.fold_in(key, 6), axis_at), (shards_of,), jnp.float32, least / len(cuts), high / len(cuts))
        level = level * jnp.repeat(jnp.exp(heights), shape[axis_at] // shards_of).reshape((-1,) + (1,) * (len(shape) - 1 - axis_at))
    return level


def noise(rng, shape, deviation, limit, cuts=(), dtype=jnp.bfloat16):
    values = jax.random.normal(rng, shape, jnp.float32) * deviation
    if len(cuts) > 0:
        values = steps_of(rng, shape, cuts, -0.22, 0.18) * values
    return jnp.clip(values, min=-limit, max=limit).astype(dtype)


def heavy_noise(own_key, shape, deviation, limit, pieces, heavy, kind=jnp.bfloat16):
    array = deviation * jax.random.normal(own_key, shape, jnp.float32)
    if pieces:
        array = array * steps_of(own_key, shape, pieces, -0.22, 0.18)
    return jnp.clip(strengthened(array, jax.random.fold_in(own_key, 3), *heavy), -limit, limit).astype(kind)


def setup_inputs(seed: int = 0) -> dict:
    keys = jax.random.split(jax.random.key(seed), 12)
    out_first = noise(keys[0], (IMAGES, SEQ, D), 1.0, 6.0, ((0, 64), (2, 4)))
    out_second = noise(keys[1], (IMAGES, SEQ, D), 1.0, 6.0, ((0, 64), (2, 4)))
    grad_first = noise(keys[2], (IMAGES, SEQ, D), 1.0, 6.0, ((0, 64), (2, 4)))
    grad_second = heavy_noise(keys[3], (IMAGES, SEQ, D), 1.0, 16.0, ((0, 64), (2, 4)), (0, 2, 64, 4.0))
    gain_attn = jnp.clip(1.0 + 0.15 * jax.random.normal(keys[4], (D,), jnp.float32), 0.25, 1.75)
    gain_mlp = jnp.clip(1.0 + 0.15 * jax.random.normal(keys[5], (D,), jnp.float32), 0.25, 1.75)
    qkv_weight = draw_qkv_weight(jax.random.fold_in(keys[11], 71), 0)
    proj_weight = noise(keys[7], (D, D), D ** -0.5, 0.1875, ((1, 4),))
    inner_weight = noise(keys[8], (D, FF), D ** -0.5, 0.1875, ((1, 4),))
    inner_bias = noise(keys[9], (FF,), 0.5, 3.0, ((0, 4),), jnp.float32)
    outer_weight = noise(keys[10], (D, FF), FF ** -0.5, 0.09375, ((1, 4),))
    return {"out_first": out_first, "out_second": out_second, "grad_first": grad_first, "grad_second": grad_second, "gain_attn": gain_attn, "gain_mlp": gain_mlp, "qkv_weight": qkv_weight, "proj_weight": proj_weight, "inner_weight": inner_weight, "inner_bias": inner_bias, "outer_weight": outer_weight}


epsilon = 1e-06

def normalize(values):
    centre = values - lax.optimization_barrier(jnp.mean(values, -1, keepdims=True))
    spread = lax.rsqrt(lax.optimization_barrier(jnp.mean(centre * centre, -1, keepdims=True)) + epsilon)
    return (centre * spread, spread)

def norm_back(grad_in, normed, spread, gain):
    scaled = grad_in * gain
    first_mean = lax.optimization_barrier(jnp.mean(scaled, -1, keepdims=True))
    second_mean = lax.optimization_barrier(jnp.mean(scaled * normed, -1, keepdims=True))
    return spread * (scaled - first_mean - normed * second_mean)

def image_attention(members):
    queries = members[0].astype(jnp.float32)
    key_rows = members[1].astype(jnp.float32)
    value_rows = members[2].astype(jnp.float32)
    grad_heads = members[3].astype(jnp.float32)
    factor = (D // HEADS) ** (-0.5)
    scores = jnp.einsum('qhe,khe->hqk', queries, key_rows) * factor
    attn_probs = jax.nn.softmax(scores, -1)
    probs_low = attn_probs.astype(jnp.bfloat16)
    probs_wide = probs_low.astype(jnp.float32)
    heads_out = jnp.einsum('hqk,khe->qhe', probs_wide, value_rows).astype(jnp.bfloat16)
    grad_probs = jnp.einsum('qhe,khe->hqk', grad_heads, value_rows)
    grad_value = jnp.einsum('hqk,qhe->khe', probs_wide, grad_heads).astype(jnp.bfloat16)
    row_dot = lax.optimization_barrier(jnp.sum(grad_probs * attn_probs, -1, keepdims=True))
    grad_scores = (attn_probs * (grad_probs - row_dot)).astype(jnp.bfloat16).astype(jnp.float32)
    grad_query = (jnp.einsum('hqk,khe->qhe', grad_scores, key_rows) * factor).astype(jnp.bfloat16)
    grad_key = (jnp.einsum('hqk,qhe->khe', grad_scores, queries) * factor).astype(jnp.bfloat16)
    return (heads_out, grad_query, grad_key, grad_value)

def reference(out_first, out_second, grad_first, grad_second, gain_attn, gain_mlp, qkv_weight, proj_weight, inner_weight, inner_bias, outer_weight):
    rows_all = IMAGES * SEQ
    head_dim = D // HEADS
    first_rows = out_first.reshape(rows_all, D).astype(jnp.float32)
    second_rows = out_second.reshape(rows_all, D).astype(jnp.float32)
    upper_grad = grad_first.reshape(rows_all, D).astype(jnp.float32)
    lower_grad = grad_second.reshape(rows_all, D)
    normed_mlp, spread_mlp = normalize(first_rows)
    input_mlp = (normed_mlp * gain_mlp).astype(jnp.bfloat16)
    hidden = jnp.dot(input_mlp, inner_weight, preferred_element_type=jnp.float32) + inner_bias
    active = jax.nn.gelu(hidden).astype(jnp.bfloat16)
    mlp_out = jnp.dot(active, outer_weight.T, preferred_element_type=jnp.float32)
    input_second = (second_rows - mlp_out).astype(jnp.bfloat16)
    grad_active = jnp.dot(lower_grad, outer_weight, preferred_element_type=jnp.float32)
    grad_hidden = jax.vjp(jax.nn.gelu, hidden)[1](grad_active)[0].astype(jnp.bfloat16)
    grad_outer = jnp.dot(lower_grad.T, active, preferred_element_type=jnp.float32)
    grad_inner = jnp.dot(input_mlp.T, grad_hidden, preferred_element_type=jnp.float32)
    grad_bias = lax.optimization_barrier(jnp.sum(grad_hidden.astype(jnp.float32), 0))
    grad_norm_mlp = jnp.dot(grad_hidden, inner_weight.T, preferred_element_type=jnp.float32)
    grad_gain_mlp = lax.optimization_barrier(jnp.sum(grad_norm_mlp * normed_mlp, 0))
    back_first = (upper_grad + norm_back(grad_norm_mlp, normed_mlp, spread_mlp, gain_mlp)).astype(jnp.bfloat16)
    normed_attn, spread_attn = normalize(input_second.astype(jnp.float32))
    input_attn = (normed_attn * gain_attn).astype(jnp.bfloat16)
    qkv_rows = jnp.einsum('td,dcj->tcj', input_attn.astype(jnp.float32), qkv_weight.astype(jnp.float32)).astype(jnp.bfloat16)
    grad_heads = jnp.dot(back_first, proj_weight, preferred_element_type=jnp.float32).astype(jnp.bfloat16)
    shaped = qkv_rows.reshape(IMAGES, SEQ, 3, HEADS, head_dim)
    heads_out, grad_query, grad_key, grad_value = lax.map(image_attention, (shaped[:, :, 0], shaped[:, :, 1], shaped[:, :, 2], grad_heads.reshape(IMAGES, SEQ, HEADS, head_dim)))
    attn_rows = heads_out.reshape(rows_all, D)
    grad_rows = jnp.stack([grad_query, grad_key, grad_value], 2).reshape(rows_all, 3, D)
    attn_out = jnp.dot(attn_rows, proj_weight.T, preferred_element_type=jnp.float32)
    input_first = (first_rows - attn_out).astype(jnp.bfloat16)
    grad_proj = jnp.dot(back_first.T, attn_rows, preferred_element_type=jnp.float32)
    grad_qkv = jnp.einsum('td,tcj->dcj', input_attn.astype(jnp.float32), grad_rows.astype(jnp.float32))
    grad_norm_attn = jnp.einsum('tcj,dcj->td', grad_rows.astype(jnp.float32), qkv_weight.astype(jnp.float32))
    grad_gain_attn = lax.optimization_barrier(jnp.sum(grad_norm_attn * normed_attn, 0))
    back_second = (lower_grad.astype(jnp.float32) + norm_back(grad_norm_attn, normed_attn, spread_attn, gain_attn)).astype(jnp.bfloat16)
    shape_out = (IMAGES, SEQ, D)
    return (input_first.reshape(shape_out), input_second.reshape(shape_out), back_first.reshape(shape_out), back_second.reshape(shape_out), grad_qkv, grad_proj, grad_inner, grad_bias, grad_outer, grad_gain_attn, grad_gain_mlp)
```

```python
import jax
import jax.numpy as jnp
from jax import lax
from jax.experimental import pallas as pl
from jax.experimental.pallas import tpu as pltpu
from jax.sharding import Mesh
from jax.sharding import PartitionSpec as P

D = 1024
HEADS = 16
AXES = ("z", "ylo", "x", "yhi", "core")
DP = ("z", "ylo", "x")
TENSOR = ("yhi", "core")
SWAP = [(0, 1), (1, 0)]
BF = jnp.bfloat16
F32 = jnp.float32
SEQ = 197
ROWS = 208
WIDTH = 256
HALF = 512
HEAD_DIM = 64
FACTOR = HEAD_DIM ** (-0.5)

epsilon = 1e-06


def swap(x, axis):
    return lax.ppermute(x, axis, SWAP)


def pick(index, zero, one):
    return jnp.where(index == 0, zero, one)


def normalize(values):
    centre = values - jnp.mean(values, -1, keepdims=True)
    spread = lax.rsqrt(jnp.mean(centre * centre, -1, keepdims=True) + epsilon)
    return (centre * spread, spread)


def norm_back(grad_in, normed, spread, gain):
    scaled = grad_in * gain
    first_mean = jnp.mean(scaled, -1, keepdims=True)
    second_mean = jnp.mean(scaled * normed, -1, keepdims=True)
    return spread * (scaled - first_mean - normed * second_mean)


def dot(a, b):
    return jnp.dot(a, b, preferred_element_type=F32)


def dot_t(a, b):
    return lax.dot_general(a, b, (((1,), (1,)), ((), ())), preferred_element_type=F32)


def t_dot(a, b):
    return lax.dot_general(a, b, (((0,), (0,)), ((), ())), preferred_element_type=F32)


def gelu_both(h):
    c = (2.0 / jnp.pi) ** 0.5
    square = h * h
    bent = jnp.tanh(c * h * (1.0 + 0.044715 * square))
    half = 0.5 * (1.0 + bent)
    slope = half + 0.5 * h * (1.0 - bent * bent) * (c * (1.0 + 3.0 * 0.044715 * square))
    return h * half, slope


def at_rows():
    return lax.broadcasted_iota(jnp.int32, (ROWS, 1), 0)


def columns(start, width):
    return pl.ds(pl.multiple_of(start, 128), width)


VMEM = pl.BlockSpec(memory_space=pltpu.VMEM)
SMEM = pl.BlockSpec(memory_space=pltpu.SMEM)


def call(kernel, outs, scratch, flops, *args):
    return pl.pallas_call(
        kernel,
        out_shape=[jax.ShapeDtypeStruct(s, d) for s, d in outs],
        in_specs=[SMEM] + [VMEM] * (len(args) - 1),
        out_specs=[VMEM] * len(outs),
        scratch_shapes=scratch,
        cost_estimate=pl.CostEstimate(flops=flops, bytes_accessed=4 << 20, transcendentals=0),
        compiler_params=pltpu.CompilerParams(vmem_limit_bytes=48 << 20),
    )(*args)


def mlp_kernel(
    at, f0, f1, f2, f3, l0, l1, l2, l3, second, upper, gain, inner, bias, outer,
    keep, away, left_in, left_out, right_in, right_out, bias_part, whole, part,
):
    tensor, core = at[0], at[1]
    half = columns(core * HALF, HALF)
    rest = columns((1 - core) * HALF, HALF)
    real = at_rows() < SEQ

    def gathered(blocks):
        whole[192:ROWS, :] = jnp.zeros((ROWS - 192, D), F32)
        for k, b in enumerate(blocks):
            whole[0:SEQ, columns((tensor ^ k) * WIDTH, WIDTH)] = b[...].astype(F32)
        return whole[...]

    def shared(values, k):
        part[...] = values
        keep[:, k * HALF : (k + 1) * HALF] = part[:, half]
        away[:, k * HALF : (k + 1) * HALF] = part[:, rest].astype(BF)

    normed, spread = normalize(gathered((f0, f1, f2, f3)))
    given = (normed * gain[...]).astype(BF)
    left_in[...] = given
    hidden = dot(given, inner[...]) + bias[...]
    active, slope = gelu_both(hidden)
    active = active.astype(BF)
    right_out[...] = active
    part[...] = -dot_t(active, outer[...])
    mine = columns(tensor * WIDTH, WIDTH)
    part[0:SEQ, mine] = part[0:SEQ, mine] + second[...].astype(F32)
    keep[:, 0:HALF] = part[:, half]
    away[:, 0:HALF] = part[:, rest].astype(BF)

    lower = gathered((l0, l1, l2, l3)).astype(BF)
    left_out[...] = lower
    grad_hidden = (dot(lower, outer[...]) * slope).astype(BF)
    right_in[...] = grad_hidden
    bias_part[...] = jnp.sum(grad_hidden.astype(F32), 0, keepdims=True)
    grad_norm = dot_t(grad_hidden, inner[...])
    gain_part = jnp.sum(grad_norm * normed, 0, keepdims=True)
    back = norm_back(grad_norm, normed, spread, gain[...])
    part[...] = jnp.where(at_rows() == SEQ, gain_part, back)
    part[0:SEQ, mine] = part[0:SEQ, mine] + upper[...].astype(F32)
    keep[:, HALF:D] = part[:, half]
    away[:, HALF:D] = part[:, rest].astype(BF)


def attention_kernel(
    at, done, theirs, gain, qkv, proj,
    left_in, left_out, rows_out, normed_out, spread_out, second_out, back_out, gain_out, whole,
):
    tensor, core = at[0], at[1]
    mine = columns(tensor * WIDTH, WIDTH)
    half = columns(core * HALF, HALF)
    rest = columns((1 - core) * HALF, HALF)
    real = at_rows() < SEQ

    whole[:, half] = done[:, 0:HALF].astype(F32)
    whole[:, rest] = theirs[:, 0:HALF].astype(F32)
    second_out[...] = whole[0:SEQ, mine].astype(BF)
    normed, spread = normalize(jnp.where(real, whole[...], 0.0))
    normed_out[...] = normed
    spread_out[...] = spread
    given = (normed * gain[...]).astype(BF)
    left_in[...] = given
    whole[:, half] = done[:, HALF:D].astype(F32)
    whole[:, rest] = theirs[:, HALF:D].astype(F32)
    back_out[...] = whole[0:SEQ, mine].astype(BF)
    gain_out[...] = whole[192:200, mine]
    back = jnp.where(real, whole[...], 0.0).astype(BF)
    left_out[...] = back

    rows = dot(given, qkv[...]).astype(BF)
    grads = dot(back, proj[...]).astype(BF)
    valid = lax.broadcasted_iota(jnp.int32, (1, ROWS), 1) < SEQ
    query_parts, key_parts, value_parts, out_parts = [], [], [], []
    for h in range(4):
        s = slice(h * HEAD_DIM, (h + 1) * HEAD_DIM)
        q = rows[:, 0:WIDTH][:, s]
        k = rows[:, WIDTH : 2 * WIDTH][:, s]
        v = rows[:, 2 * WIDTH :][:, s]
        g = grads[:, s]
        scores = jnp.where(valid, dot_t(q, k) * FACTOR, -1e30)
        raised = jnp.exp(scores - jnp.max(scores, -1, keepdims=True))
        probs = raised / jnp.sum(raised, -1, keepdims=True)
        low = probs.astype(BF)
        out_parts.append(dot(low, v))
        grad_probs = dot_t(g, v)
        value_parts.append(t_dot(low, g))
        row_dot = jnp.sum(grad_probs * probs, -1, keepdims=True)
        grad_scores = (probs * (grad_probs - row_dot)).astype(BF)
        query_parts.append(dot(grad_scores, k) * FACTOR)
        key_parts.append(t_dot(grad_scores, q) * FACTOR)
    for n, parts in enumerate((query_parts, key_parts, value_parts, out_parts)):
        rows_out[:, n * WIDTH : (n + 1) * WIDTH] = jnp.concatenate(parts, 1).astype(BF)


def close_kernel(at, rows, normed, spread, gain, qkv, proj, keep, away, part):
    core = at[1]

    def quarters(first_column):
        for k in range(2):
            to = slice(first_column + k * WIDTH, first_column + (k + 1) * WIDTH)
            keep[:, to] = part[:, columns((2 * k + core) * WIDTH, WIDTH)]
            away[:, to] = part[:, columns((2 * k + 1 - core) * WIDTH, WIDTH)].astype(BF)

    grad_norm = dot_t(rows[:, 0 : 3 * WIDTH], qkv[...])
    gain_part = jnp.sum(grad_norm * normed[...], 0, keepdims=True)
    back = norm_back(grad_norm, normed[...], spread[...], gain[...])
    part[...] = jnp.where(at_rows() == SEQ, gain_part, back)
    quarters(HALF)
    part[...] = dot_t(rows[:, 3 * WIDTH :], proj[...])
    quarters(0)


def products_kernel(widths, extra, at, *refs):
    n = len(widths)
    lefts, rights = refs[:n], refs[n : 2 * n]
    small = refs[2 * n] if extra else None
    outs = refs[2 * n + extra : 2 * n + extra + 4]
    turned, chosen = refs[-2:]
    x = at[2]
    column = 0
    for left, right, width in zip(lefts, rights, widths):
        turned[...] = left[...].astype(F32).T.astype(BF)
        for k in range(4):
            owner = (x + k) % 4
            for b in range(16):
                chosen[b * 16 : (b + 1) * 16, :] = turned[
                    pl.ds(pl.multiple_of(b * 64 + owner * 16, 16), 16), :
                ]
            outs[k][:, column : column + width] = dot(chosen[...], right[...]).astype(BF)
        column += width
    if extra:
        block = jnp.concatenate([small[...], jnp.zeros((24, 128), F32)], 0).astype(BF)
        for k in range(4):
            for b in range(8):
                outs[k][b * 32 : (b + 1) * 32, column:] = block


def products(at, lefts, rights, widths, small=None):
    total = sum(widths) + (128 if small is not None else 0)
    args = (at, *lefts, *rights) + ((small,) if small is not None else ())

    def kernel(*refs):
        products_kernel(widths, int(small is not None), *refs)

    return call(
        kernel,
        [((256, total), BF)] * 4,
        [pltpu.VMEM((D, ROWS), BF), pltpu.VMEM((256, ROWS), BF)],
        2 * D * ROWS * total,
        *args,
    )


def around(axis_size, step):
    return [(i, (i + step) % axis_size) for i in range(axis_size)]


def over_x(pieces):
    came = [lax.ppermute(pieces[k], "x", around(4, k)) for k in (1, 2, 3)]
    return sum((c.astype(F32) for c in came), pieces[0].astype(F32))


def over_z(total):
    came = lax.all_to_all(total.astype(BF).reshape(8, 32, -1), "z", 0, 0, tiled=True)
    return jnp.sum(came.astype(F32), 0)


def over_ylo(rows, ylo, main):
    keep = pick(ylo, rows[:16, :main], rows[16:, :main])
    away = pick(ylo, rows[16:, :main], rows[:16, :main])
    small = rows[:16, main:]
    came = swap(jnp.concatenate([away, small], 1).astype(BF), "ylo").astype(F32)
    return keep + came[:, :main], small + came[:, main:]


def on_device(
    out_first,
    out_second,
    grad_first,
    grad_second,
    gain_attn,
    gain_mlp,
    qkv_weight,
    proj_weight,
    inner_weight,
    inner_bias,
    outer_weight,
):
    yhi, core, ylo, x = (lax.axis_index(a) for a in ("yhi", "core", "ylo", "x"))
    at = jnp.stack([yhi * 2 + core, core, x, ylo]).astype(jnp.int32)
    first, second, upper, lower = (
        a.reshape(SEQ, WIDTH) for a in (out_first, out_second, grad_first, grad_second)
    )
    gain_m, gain_a = gain_mlp.reshape(1, D), gain_attn.reshape(1, D)
    flat_qkv = qkv_weight.reshape(D, 3 * WIDTH)
    block = (ROWS, D)

    def gather(own):
        by_core, by_yhi = swap(own, "core"), swap(own, "yhi")
        return own, by_core, by_yhi, swap(by_yhi, "core")

    keep, away, left_in, left_out, right_in, right_out, bias_part = call(
        mlp_kernel,
        [(block, F32), (block, BF), (block, BF), (block, BF), (block, BF), (block, BF), ((1, D), F32)],
        [pltpu.VMEM(block, F32), pltpu.VMEM(block, F32)],
        8 * ROWS * D * D,
        at,
        *gather(first),
        *gather(lower),
        second,
        upper,
        gain_m,
        inner_weight,
        inner_bias.reshape(1, D),
        outer_weight,
    )
    come = swap(away, "core")
    pair = (keep + come.astype(F32)).astype(BF)
    other = swap(pair, "yhi")
    done = (pair.astype(F32) + other.astype(F32)).astype(BF)
    theirs = swap(done, "core")

    mlp_pieces = products(
        at, (left_in, left_out), (right_in, right_out), (D, D), bias_part.reshape(8, 128)
    )
    mlp_rows, mlp_small = over_ylo(over_z(over_x(mlp_pieces)), ylo, 2 * D)

    attn_in, attn_back, rows, normed, spread, input_second, back_first, gain_rows = call(
        attention_kernel,
        [
            (block, BF),
            (block, BF),
            (block, BF),
            (block, F32),
            ((ROWS, 1), F32),
            ((SEQ, WIDTH), BF),
            ((SEQ, WIDTH), BF),
            ((8, WIDTH), F32),
        ],
        [pltpu.VMEM(block, F32)],
        4 * ROWS * D * D,
        at,
        done,
        theirs,
        gain_a,
        flat_qkv,
        proj_weight,
    )
    attn_pieces = products(
        at, (attn_in, attn_back), (rows[:, : 3 * WIDTH], rows[:, 3 * WIDTH :]), (3 * WIDTH, WIDTH)
    )
    keep, away = call(
        close_kernel,
        [(block, F32), (block, BF)],
        [pltpu.VMEM(block, F32)],
        2 * ROWS * D * D,
        at,
        rows,
        normed,
        spread,
        gain_a,
        flat_qkv,
        proj_weight,
    )
    pair = keep + swap(away, "core").astype(F32)
    mine = jnp.concatenate([pick(yhi, pair[:, a : a + WIDTH], pair[:, a + WIDTH : a + HALF]) for a in (0, HALF)], 1)
    sent = jnp.concatenate([pick(yhi, pair[:, a + WIDTH : a + HALF], pair[:, a : a + WIDTH]) for a in (0, HALF)], 1)
    closed = mine + swap(sent.astype(BF), "yhi").astype(F32)
    input_first = (first.astype(F32) - closed[:SEQ, :WIDTH]).astype(BF)
    back_second = (lower.astype(F32) + closed[:SEQ, WIDTH:]).astype(BF)

    gains = jnp.concatenate([closed[SEQ, WIDTH:].reshape(2, 128), gain_rows[5].reshape(2, 128)], 0)
    gains = over_x([gains] * 4)
    gain_block = jnp.tile(jnp.concatenate([gains, jnp.zeros((28, 128), F32)], 0), (8, 1))
    attn_rows, attn_small = over_ylo(
        over_z(jnp.concatenate([over_x(attn_pieces), gain_block], 1)), ylo, D
    )

    shape_out = (1, SEQ, WIDTH)
    return (
        input_first.reshape(shape_out),
        input_second.reshape(shape_out),
        back_first.reshape(shape_out),
        back_second.reshape(shape_out),
        attn_rows[:, : 3 * WIDTH].reshape(16, 3, WIDTH),
        attn_rows[:, 3 * WIDTH :],
        mlp_rows[:, :D],
        mlp_small[:8].reshape(D),
        mlp_rows[:, D:],
        attn_small[0:2].reshape(WIDTH),
        attn_small[2:4].reshape(WIDTH),
    )


def solution(mesh):
    split = Mesh(mesh.devices.reshape(8, 2, 4, 2, 2), AXES)
    rows = P(DP, None, TENSOR)
    return jax.shard_map(
        on_device,
        mesh=split,
        in_specs=(
            rows,
            rows,
            rows,
            rows,
            P(),
            P(),
            P(None, None, TENSOR),
            P(None, TENSOR),
            P(None, TENSOR),
            P(TENSOR),
            P(None, TENSOR),
        ),
        out_specs=(
            rows,
            rows,
            rows,
            rows,
            rows,
            P(DP, TENSOR),
            P(DP, TENSOR),
            P(TENSOR),
            P(DP, TENSOR),
            P(TENSOR),
            P(TENSOR),
        ),
        check_vma=False,
    )
```

```python
import jax
import jax.numpy as jnp
from jax import lax
from jax.experimental import pallas as pl
from jax.experimental.pallas import tpu as pltpu
from jax.sharding import Mesh
from jax.sharding import PartitionSpec as P

D = 1024
AXES = ("z", "ylo", "x", "yhi", "core")
DP = ("z", "ylo", "x")
TENSOR = ("yhi", "core")
SWAP = [(0, 1), (1, 0)]
BF = jnp.bfloat16
F32 = jnp.float32
SEQ = 197
ROWS = 208
WIDTH = 256
HALF = 512
WIDE = 2 * D
STEPS = (2, 1, 3, 0)
HEAD_DIM = 64
FACTOR = HEAD_DIM ** (-0.5)

epsilon = 1e-06


def swap(x, axis):
    return lax.ppermute(x, axis, SWAP)


def around(x, step):
    return lax.ppermute(x, "x", [(i, (i + step) % 4) for i in range(4)])


def normalize(values):
    centre = values - jnp.mean(values, -1, keepdims=True)
    spread = lax.rsqrt(jnp.mean(centre * centre, -1, keepdims=True) + epsilon)
    return (centre * spread, spread)


def norm_back(grad_in, normed, spread, gain):
    scaled = grad_in * gain
    first_mean = jnp.mean(scaled, -1, keepdims=True)
    second_mean = jnp.mean(scaled * normed, -1, keepdims=True)
    return spread * (scaled - first_mean - normed * second_mean)


def dot(a, b):
    return jnp.dot(a, b, preferred_element_type=F32)


def dot_t(a, b):
    return lax.dot_general(a, b, (((1,), (1,)), ((), ())), preferred_element_type=F32)


def t_dot(a, b):
    return lax.dot_general(a, b, (((0,), (0,)), ((), ())), preferred_element_type=F32)


def gelu_both(h):
    c = (2.0 / jnp.pi) ** 0.5
    square = h * h
    bent = jnp.tanh(c * h * (1.0 + 0.044715 * square))
    half = 0.5 * (1.0 + bent)
    slope = half + 0.5 * h * (1.0 - bent * bent) * (c * (1.0 + 3.0 * 0.044715 * square))
    return h * half, slope


def at_rows():
    return lax.broadcasted_iota(jnp.int32, (ROWS, 1), 0)


def columns(start, width):
    return pl.ds(pl.multiple_of(start, 128), width)


VMEM = pl.BlockSpec(memory_space=pltpu.VMEM)
SMEM = pl.BlockSpec(memory_space=pltpu.SMEM)
ANY = pl.BlockSpec(memory_space=pl.ANY)


def call(kernel, outs, scratch, flops, *args, limit=20):
    return pl.pallas_call(
        kernel,
        out_shape=[jax.ShapeDtypeStruct(s, d) for s, d in outs],
        in_specs=[SMEM] + [VMEM] * (len(args) - 1),
        out_specs=[VMEM] * len(outs),
        scratch_shapes=scratch,
        cost_estimate=pl.CostEstimate(flops=flops, bytes_accessed=4 << 20, transcendentals=0),
        compiler_params=pltpu.CompilerParams(vmem_limit_bytes=limit << 20),
    )(*args)


def pause_kernel(out):
    out[...] = jnp.zeros((8, 128), F32)


def pause(size):
    return pl.pallas_call(
        pause_kernel,
        out_shape=jax.ShapeDtypeStruct((8, 128), F32),
        out_specs=VMEM,
        cost_estimate=pl.CostEstimate(flops=size, bytes_accessed=size >> 13, transcendentals=0),
        compiler_params=pltpu.CompilerParams(vmem_limit_bytes=1 << 20),
    )()


def pass_kernel(values, out):
    out[...] = values[...]


def passed(values):
    return pl.pallas_call(
        pass_kernel,
        out_shape=jax.ShapeDtypeStruct(values.shape, values.dtype),
        in_specs=[VMEM],
        out_specs=VMEM,
        cost_estimate=pl.CostEstimate(flops=8 << 30, bytes_accessed=1 << 20, transcendentals=0),
        compiler_params=pltpu.CompilerParams(vmem_limit_bytes=1 << 20),
    )(values)


def mlp_kernel(
    at, f0, f1, f2, f3, l0, l1, l2, l3, second, upper, vectors, inner, outer, mark,
    keep, away, left_in, left_out, right, bias_part, whole, part,
):
    tensor, core = at[0], at[1]
    half = columns(core * HALF, HALF)
    rest = columns((1 - core) * HALF, HALF)
    gain, bias = vectors[0:1, :], vectors[1:2, :]

    def gathered(blocks):
        whole[192:ROWS, :] = jnp.zeros((ROWS - 192, D), F32)
        for k, b in enumerate(blocks):
            whole[0:SEQ, columns((tensor ^ k) * WIDTH, WIDTH)] = b[...].astype(F32)
        return whole[...]

    normed, spread = normalize(gathered((f0, f1, f2, f3)))
    given = (normed * gain).astype(BF)
    left_in[...] = given
    hidden = dot(given, inner[...]) + bias
    active, slope = gelu_both(hidden)
    active = active.astype(BF)
    right[:, D:] = active
    part[...] = -dot_t(active, outer[...])
    mine = columns(tensor * WIDTH, WIDTH)
    part[0:SEQ, mine] = part[0:SEQ, mine] + second[...].astype(F32)
    keep[:, 0:HALF] = part[:, half]
    away[:, 0:HALF] = part[:, rest].astype(BF)

    lower = gathered((l0, l1, l2, l3)).astype(BF)
    left_out[...] = lower
    grad_hidden = (dot(lower, outer[...]) * slope).astype(BF)
    right[:, :D] = grad_hidden
    bias_part[...] = jnp.sum(grad_hidden.astype(F32), 0, keepdims=True)
    grad_norm = dot_t(grad_hidden, inner[...])
    gain_part = jnp.sum(grad_norm * normed, 0, keepdims=True)
    back = norm_back(grad_norm, normed, spread, gain)
    part[...] = jnp.where(at_rows() == SEQ, gain_part, back)
    part[0:SEQ, mine] = part[0:SEQ, mine] + upper[...].astype(F32)
    keep[:, HALF:D] = part[:, half]
    away[:, HALF:D] = part[:, rest].astype(BF)


def before_kernel(
    at, done, theirs, gain, mark,
    given_out, back_in, normed_out, spread_out, second_out, back_out, gain_out, keep, away, whole, turned,
):
    tensor, core = at[0], at[1]
    mine = columns(tensor * WIDTH, WIDTH)
    half = columns(core * HALF, HALF)
    rest = columns((1 - core) * HALF, HALF)
    real = at_rows() < SEQ

    def sorted_rows(values, first):
        turned[...] = values.T.astype(BF)
        for out, y in ((keep, at[3]), (away, 1 - at[3])):
            for to, (k, z) in enumerate((k, z) for k in STEPS for z in range(8)):
                row = (z * 8 + y * 4 + (at[2] + k) % 4) * 16
                out[first + to * 16 : first + (to + 1) * 16, :] = turned[pl.ds(pl.multiple_of(row, 16), 16), :]

    whole[:, half] = done[:, 0:HALF].astype(F32)
    whole[:, rest] = theirs[:, 0:HALF].astype(F32)
    second_out[...] = whole[0:SEQ, mine].astype(BF)
    normed, spread = normalize(jnp.where(real, whole[...], 0.0))
    normed_out[...] = normed
    spread_out[...] = spread
    given = (normed * gain[...]).astype(BF)
    given_out[...] = given
    sorted_rows(given.astype(F32), 0)
    whole[:, half] = done[:, HALF:D].astype(F32)
    whole[:, rest] = theirs[:, HALF:D].astype(F32)
    back_out[...] = whole[0:SEQ, mine].astype(BF)
    gain_out[...] = whole[192:200, mine]
    back = jnp.where(real, whole[...], 0.0)
    back_in[...] = back.astype(BF)
    sorted_rows(back, 512)


def attention_kernel(at, given, back, qkv, proj, rows_out):
    rows = [dot(given[...], qkv[c]).astype(BF) for c in range(3)]
    grads = dot(back[...], proj[...]).astype(BF)
    valid = lax.broadcasted_iota(jnp.int32, (1, ROWS), 1) < SEQ
    query_parts, key_parts, value_parts, out_parts = [], [], [], []
    for h in range(4):
        s = slice(h * HEAD_DIM, (h + 1) * HEAD_DIM)
        q, k, v = (r[:, s] for r in rows)
        g = grads[:, s]
        scores = jnp.where(valid, dot_t(q, k) * FACTOR, -1e30)
        raised = jnp.exp(scores - jnp.max(scores, -1, keepdims=True))
        probs = raised / jnp.sum(raised, -1, keepdims=True)
        low = probs.astype(BF)
        out_parts.append(dot(low, v))
        grad_probs = dot_t(g, v)
        value_parts.append(t_dot(low, g))
        row_dot = jnp.sum(grad_probs * probs, -1, keepdims=True)
        grad_scores = (probs * (grad_probs - row_dot)).astype(BF)
        query_parts.append(dot(grad_scores, k) * FACTOR)
        key_parts.append(t_dot(grad_scores, q) * FACTOR)
    for n, parts in enumerate((query_parts, key_parts, value_parts, out_parts)):
        rows_out[:, n * WIDTH : (n + 1) * WIDTH] = jnp.concatenate(parts, 1).astype(BF)


def close_kernel(at, rows, normed, spread, gain, qkv, proj, keep, away, part):
    core = at[1]

    def quarters(first_column):
        for k in range(2):
            to = slice(first_column + k * WIDTH, first_column + (k + 1) * WIDTH)
            keep[:, to] = part[:, columns((2 * k + core) * WIDTH, WIDTH)]
            away[:, to] = part[:, columns((2 * k + 1 - core) * WIDTH, WIDTH)].astype(BF)

    grad_norm = sum(dot_t(rows[:, c * WIDTH : (c + 1) * WIDTH], qkv[c]) for c in range(3))
    gain_part = jnp.sum(grad_norm * normed[...], 0, keepdims=True)
    back = norm_back(grad_norm, normed[...], spread[...], gain[...])
    part[...] = jnp.where(at_rows() == SEQ, gain_part, back)
    quarters(HALF)
    part[...] = dot_t(rows[:, 3 * WIDTH :], proj[...])
    quarters(0)


def close_pair_kernel(at, keep, came, mine, sent):
    yhi = at[0] // 2
    for k in range(2):
        to = slice(k * WIDTH, (k + 1) * WIDTH)
        low, high = (
            keep[:, c : c + WIDTH] + came[:, c : c + WIDTH].astype(F32)
            for c in (k * HALF, k * HALF + WIDTH)
        )
        mine[:, to] = jnp.where(yhi == 0, low, high)
        sent[:, to] = jnp.where(yhi == 0, high, low).astype(BF)


def close_end_kernel(at, mine, came, first, lower, gain_m, bias, input_first, back_second, small):
    total = mine[...] + came[...].astype(F32)
    input_first[...] = (first[...].astype(F32) - total[0:SEQ, :WIDTH]).astype(BF)
    back_second[...] = (lower[...].astype(F32) + total[0:SEQ, WIDTH:]).astype(BF)
    row = total[192:200, WIDTH:]
    small[0:8, :] = bias[...]
    for k in range(2):
        small[8 + k : 9 + k, :] = row[5:6, k * 128 : (k + 1) * 128]
        small[10 + k : 11 + k, :] = gain_m[5:6, k * 128 : (k + 1) * 128]


def turn(left, turned):
    turned[...] = left[...].astype(F32).T.astype(BF)


def rows_of(turned, chosen, blocks):
    for to, b in enumerate(blocks):
        chosen[to * 16 : (to + 1) * 16, :] = turned[pl.ds(pl.multiple_of(b * 16, 16), 16), :]
    return chosen[...]


def far_kernel(at, left_in, left_out, right, far_a, far_b, turned_in, turned_out, chosen):
    turn(left_in, turned_in)
    turn(left_out, turned_out)
    blocks = [b * 4 + (at[2] + 2) % 4 for b in range(16)]
    far_a[...] = dot(rows_of(turned_in, chosen, blocks), right[:, :D]).astype(BF)
    far_b[...] = dot(rows_of(turned_out, chosen, blocks), right[:, D:]).astype(BF)


def near_kernel(at, turned_in, turned_out, right, a1, b1, a3, b3, a0, b0, chosen):
    for k, a, b in ((1, a1, b1), (3, a3, b3), (0, a0, b0)):
        blocks = [r * 4 + (at[2] + k) % 4 for r in range(16)]
        a[...] = dot(rows_of(turned_in, chosen, blocks), right[:, :D]).astype(BF)
        b[...] = dot(rows_of(turned_out, chosen, blocks), right[:, D:]).astype(BF)


def pieces_kernel(at, own_left, came_left, own_right, came_right, *pieces):
    for to, piece in enumerate(pieces):
        for first, low, high in ((0, 0, 3 * WIDTH), (512, 3 * WIDTH, D)):
            r = slice(first + to * 128, first + (to + 1) * 128)
            piece[:, low:high] = (
                dot(own_left[r, :], own_right[:, low:high]) + dot(came_left[r, :], came_right[:, low:high])
            ).astype(BF)


def added(a, b):
    return (a.astype(F32) + b.astype(F32)).astype(BF)


def sum_kernel(at, a0, a1, a2, b0, b1, b2, keep, away):
    split = a0.shape[1]
    for cols, terms in ((slice(0, split), (a0, a1, a2)), (slice(split, WIDE), (b0, b1, b2))):
        total = sum(t[...].astype(F32) for t in terms[1:]) + terms[0][...].astype(F32)
        for z in range(8):
            to = slice(z * 16, (z + 1) * 16)
            low, high = total[z * 32 : z * 32 + 16], total[z * 32 + 16 : z * 32 + 32]
            keep[to, cols] = jnp.where(at[3] == 0, low, high).astype(BF)
            away[to, cols] = jnp.where(at[3] == 0, high, low).astype(BF)


def merge_kernel(at, keep, came, a, b, c, d, small, total):
    total[:, :WIDE] = (keep[...].astype(F32) + came[...].astype(F32)).astype(BF)
    terms = [r[...].astype(F32) for r in (a, b, c, d)]
    total[:, WIDE : WIDE + D] = (terms[0] + terms[1] + terms[2] + terms[3]).astype(BF)
    block = jnp.concatenate([small[...], jnp.zeros((4, 128), F32)], 0).astype(BF)
    total[:, WIDE + D :] = jnp.concatenate([block] * 8, 0)


def end_kernel(at, came, inner, outer, bias, qkv, proj, gain_a, gain_m):
    total = came[0].astype(F32)
    for k in range(1, 8):
        total = total + came[k].astype(F32)
    inner[...] = total[:, :D]
    outer[...] = total[:, D:WIDE]
    for c in range(3):
        qkv[c] = total[:, WIDE + c * WIDTH : WIDE + (c + 1) * WIDTH]
    proj[...] = total[:, WIDE + 3 * WIDTH : WIDE + D]
    small = total[:, WIDE + D :]
    for k in range(8):
        bias[:, k * 128 : (k + 1) * 128] = small[k : k + 1, :]
    for k in range(2):
        gain_a[:, k * 128 : (k + 1) * 128] = small[8 + k : 9 + k, :]
        gain_m[:, k * 128 : (k + 1) * 128] = small[10 + k : 11 + k, :]


def on_device(
    out_first,
    out_second,
    grad_first,
    grad_second,
    gain_attn,
    gain_mlp,
    qkv_weight,
    proj_weight,
    inner_weight,
    inner_bias,
    outer_weight,
):
    yhi, core, ylo, x = (lax.axis_index(a) for a in ("yhi", "core", "ylo", "x"))
    at = jnp.stack([yhi * 2 + core, core, x, ylo]).astype(jnp.int32)
    first, second, upper, lower = (
        a.reshape(SEQ, WIDTH) for a in (out_first, out_second, grad_first, grad_second)
    )
    block = (ROWS, D)

    first_y, lower_y = swap(first, "yhi"), swap(lower, "yhi")
    first_c, lower_c = swap(first, "core"), swap(lower, "core")
    first_b, lower_b = swap(first_y, "core"), swap(lower_y, "core")
    gain_a = gain_attn.reshape(1, D)
    qkv = jnp.moveaxis(qkv_weight, 1, 0)
    proj = proj_weight
    keep, away, left_in, left_out, right, bias_part = call(
        mlp_kernel,
        [(block, F32), (block, BF), (block, BF), (block, BF), ((ROWS, 2 * D), BF), ((1, D), F32)],
        [pltpu.VMEM(block, F32), pltpu.VMEM(block, F32)],
        8 * ROWS * D * D,
        at,
        first,
        first_c,
        first_y,
        first_b,
        lower,
        lower_c,
        lower_y,
        lower_b,
        second,
        upper,
        passed(jnp.stack([gain_mlp, inner_bias])),
        inner_weight,
        outer_weight,
        pause(8 << 30),
    )
    come = swap(away, "core")
    pair = (keep + come.astype(F32)).astype(BF)
    other = swap(pair, "yhi")
    done = added(pair, other)
    theirs = swap(done, "core")

    far_a, far_b, turned_in, turned_out = call(
        far_kernel,
        [((256, D), BF), ((256, D), BF), ((D, ROWS), BF), ((D, ROWS), BF)],
        [pltpu.VMEM((256, ROWS), BF)],
        D * ROWS * D,
        at,
        left_in,
        left_out,
        right,
    )
    came_a, came_b = around(far_a, 1), around(far_b, -1)
    a1, b1, a3, b3, a0, b0 = call(
        near_kernel,
        [((256, D), BF)] * 6,
        [pltpu.VMEM((256, ROWS), BF)],
        3 * D * ROWS * D,
        at,
        turned_in,
        turned_out,
        right,
    )
    near_b, near_a = around(b1, 1), around(a3, -1)
    join_a, join_b = added(a1, came_a), added(b3, came_b)
    joined_a, joined_b = around(join_a, 1), around(join_b, -1)
    mlp_keep, mlp_away = call(
        sum_kernel,
        [((128, WIDE), BF)] * 2,
        [],
        1 << 24,
        at,
        a0,
        near_a,
        joined_a,
        b0,
        near_b,
        joined_b,
    )
    mlp_came = swap(mlp_away, "ylo")

    given, back, normed, spread, input_second, back_first, gain_rows, own_left, away_left = call(
        before_kernel,
        [
            (block, BF),
            (block, BF),
            (block, F32),
            ((ROWS, 1), F32),
            ((SEQ, WIDTH), BF),
            ((SEQ, WIDTH), BF),
            ((8, WIDTH), F32),
            ((D, ROWS), BF),
            ((D, ROWS), BF),
        ],
        [pltpu.VMEM(block, F32), pltpu.VMEM((D, ROWS), BF)],
        ROWS * D * D,
        at,
        done,
        theirs,
        gain_a,
        pause(1 << 20),
    )
    came_left = swap(away_left, "ylo")
    (rows,) = call(attention_kernel, [(block, BF)], [], 4 * ROWS * D * D, at, given, back, qkv, proj)
    came_rows = swap(rows, "ylo")
    keep, away = call(
        close_kernel,
        [(block, F32), (block, BF)],
        [pltpu.VMEM(block, F32)],
        2 * ROWS * D * D,
        at,
        rows,
        normed,
        spread,
        gain_a,
        qkv,
        proj,
    )
    pieces = call(
        pieces_kernel,
        [((128, D), BF)] * 4,
        [],
        2 * D * ROWS * D,
        at,
        own_left,
        came_left,
        rows,
        came_rows,
    )
    came = [around(pieces[to], k) for to, k in enumerate(STEPS[:3])]
    mine, sent = call(
        close_pair_kernel,
        [((ROWS, HALF), F32), ((ROWS, HALF), BF)],
        [],
        1 << 22,
        at,
        keep,
        swap(away, "core"),
    )
    input_first, back_second, small = call(
        close_end_kernel,
        [((SEQ, WIDTH), BF), ((SEQ, WIDTH), BF), ((12, 128), F32)],
        [],
        1 << 22,
        at,
        mine,
        swap(sent, "yhi"),
        first,
        lower,
        gain_rows,
        bias_part.reshape(8, 128),
    )
    small = small + swap(small, "ylo")
    small = small + sum(around(small, k) for k in (1, 2, 3))
    (total,) = call(
        merge_kernel,
        [((128, WIDE + D + 128), BF)],
        [],
        1 << 22,
        at,
        mlp_keep,
        mlp_came,
        pieces[3],
        *came,
        small,
    )
    came = lax.all_to_all(total.reshape(8, 16, -1), "z", 0, 0, tiled=True)
    grad_inner, grad_outer, bias_sum, grad_qkv, grad_proj, gain_a_sum, gain_m_sum = call(
        end_kernel,
        [
            ((16, D), F32),
            ((16, D), F32),
            ((1, D), F32),
            ((3, 16, WIDTH), F32),
            ((16, WIDTH), F32),
            ((1, WIDTH), F32),
            ((1, WIDTH), F32),
        ],
        [],
        1 << 20,
        at,
        came,
    )

    shape_out = (1, SEQ, WIDTH)
    return (
        input_first.reshape(shape_out),
        input_second.reshape(shape_out),
        back_first.reshape(shape_out),
        back_second.reshape(shape_out),
        jnp.moveaxis(grad_qkv, 0, 1),
        grad_proj,
        grad_inner,
        bias_sum.reshape(D),
        grad_outer,
        gain_a_sum.reshape(WIDTH),
        gain_m_sum.reshape(WIDTH),
    )


def solution(mesh):
    split = Mesh(mesh.devices.reshape(8, 2, 4, 2, 2), AXES)
    rows = P(DP, None, TENSOR)
    return jax.shard_map(
        on_device,
        mesh=split,
        in_specs=(
            rows,
            rows,
            rows,
            rows,
            P(),
            P(),
            P(None, None, TENSOR),
            P(None, TENSOR),
            P(None, TENSOR),
            P(TENSOR),
            P(None, TENSOR),
        ),
        out_specs=(
            rows,
            rows,
            rows,
            rows,
            rows,
            P(DP, TENSOR),
            P(DP, TENSOR),
            P(TENSOR),
            P(DP, TENSOR),
            P(TENSOR),
            P(TENSOR),
        ),
        check_vma=False,
    )
```

```python
import jax
import jax.numpy as jnp
from jax import lax
from jax.experimental import pallas as pl
from jax.experimental.pallas import tpu as pltpu
from jax.sharding import Mesh
from jax.sharding import PartitionSpec as P

D = 1024
AXES = ("z", "ylo", "x", "yhi", "core")
DP = ("z", "ylo", "x")
TENSOR = ("yhi", "core")
SWAP = [(0, 1), (1, 0)]
BF = jnp.bfloat16
F32 = jnp.float32
SEQ = 197
ROWS = 208
WIDTH = 256
HALF = 512
WIDE = 2 * D
STEPS = (2, 1, 3, 0)
HEAD_DIM = 64
FACTOR = HEAD_DIM ** (-0.5)

epsilon = 1e-06


def swap(x, axis):
    return lax.ppermute(x, axis, SWAP)


def around(x, step):
    return lax.ppermute(x, "x", [(i, (i + step) % 4) for i in range(4)])


def normalize(values):
    centre = values - jnp.mean(values, -1, keepdims=True)
    spread = lax.rsqrt(jnp.mean(centre * centre, -1, keepdims=True) + epsilon)
    return (centre * spread, spread)


def norm_back(grad_in, normed, spread, gain):
    scaled = grad_in * gain
    first_mean = jnp.mean(scaled, -1, keepdims=True)
    second_mean = jnp.mean(scaled * normed, -1, keepdims=True)
    return spread * (scaled - first_mean - normed * second_mean)


def dot(a, b):
    return jnp.dot(a, b, preferred_element_type=F32)


def dot_t(a, b):
    return lax.dot_general(a, b, (((1,), (1,)), ((), ())), preferred_element_type=F32)


def t_dot(a, b):
    return lax.dot_general(a, b, (((0,), (0,)), ((), ())), preferred_element_type=F32)


def gelu_both(h):
    c = (2.0 / jnp.pi) ** 0.5
    square = h * h
    bent = jnp.tanh(c * h * (1.0 + 0.044715 * square))
    half = 0.5 * (1.0 + bent)
    slope = half + 0.5 * h * (1.0 - bent * bent) * (c * (1.0 + 3.0 * 0.044715 * square))
    return h * half, slope


def at_rows():
    return lax.broadcasted_iota(jnp.int32, (ROWS, 1), 0)


def columns(start, width):
    return pl.ds(pl.multiple_of(start, 128), width)


VMEM = pl.BlockSpec(memory_space=pltpu.VMEM)
SMEM = pl.BlockSpec(memory_space=pltpu.SMEM)
ANY = pl.BlockSpec(memory_space=pl.ANY)


def call(kernel, outs, scratch, flops, *args, limit=20):
    return pl.pallas_call(
        kernel,
        out_shape=[jax.ShapeDtypeStruct(s, d) for s, d in outs],
        in_specs=[SMEM] + [VMEM] * (len(args) - 1),
        out_specs=[VMEM] * len(outs),
        scratch_shapes=scratch,
        cost_estimate=pl.CostEstimate(flops=flops, bytes_accessed=4 << 20, transcendentals=0),
        compiler_params=pltpu.CompilerParams(vmem_limit_bytes=limit << 20),
    )(*args)


def pause_kernel(out):
    out[...] = jnp.zeros((8, 128), F32)


def pause(size):
    return pl.pallas_call(
        pause_kernel,
        out_shape=jax.ShapeDtypeStruct((8, 128), F32),
        out_specs=VMEM,
        cost_estimate=pl.CostEstimate(flops=size, bytes_accessed=size >> 13, transcendentals=0),
        compiler_params=pltpu.CompilerParams(vmem_limit_bytes=1 << 20),
    )()


def pass_kernel(values, weight, out):
    out[...] = values[...]


def passed(values, weight):
    return pl.pallas_call(
        pass_kernel,
        out_shape=jax.ShapeDtypeStruct(values.shape, values.dtype),
        in_specs=[VMEM, ANY],
        out_specs=VMEM,
        cost_estimate=pl.CostEstimate(flops=8 << 30, bytes_accessed=1 << 20, transcendentals=0),
        compiler_params=pltpu.CompilerParams(vmem_limit_bytes=1 << 20),
    )(values, weight)


def mlp_kernel(
    at, f0, f1, f2, f3, l0, l1, l2, l3, second, upper, vectors, inner, outer, mark,
    keep, away, left_in, left_out, right, bias_part, whole, part,
):
    tensor, core = at[0], at[1]
    half = columns(core * HALF, HALF)
    rest = columns((1 - core) * HALF, HALF)
    gain, bias = vectors[0:1, :], vectors[1:2, :]

    def gathered(blocks):
        whole[192:ROWS, :] = jnp.zeros((ROWS - 192, D), F32)
        for k, b in enumerate(blocks):
            whole[0:SEQ, columns((tensor ^ k) * WIDTH, WIDTH)] = b[...].astype(F32)
        return whole[...]

    normed, spread = normalize(gathered((f0, f1, f2, f3)))
    given = (normed * gain).astype(BF)
    left_in[...] = given
    hidden = dot(given, inner[...]) + bias
    active, slope = gelu_both(hidden)
    active = active.astype(BF)
    right[:, D:] = active
    part[...] = -dot_t(active, outer[...])
    mine = columns(tensor * WIDTH, WIDTH)
    part[0:SEQ, mine] = part[0:SEQ, mine] + second[...].astype(F32)
    keep[:, 0:HALF] = part[:, half]
    away[:, 0:HALF] = part[:, rest].astype(BF)

    lower = gathered((l0, l1, l2, l3)).astype(BF)
    left_out[...] = lower
    grad_hidden = (dot(lower, outer[...]) * slope).astype(BF)
    right[:, :D] = grad_hidden
    bias_part[...] = jnp.sum(grad_hidden.astype(F32), 0, keepdims=True)
    grad_norm = dot_t(grad_hidden, inner[...])
    gain_part = jnp.sum(grad_norm * normed, 0, keepdims=True)
    back = norm_back(grad_norm, normed, spread, gain)
    part[...] = jnp.where(at_rows() == SEQ, gain_part, back)
    part[0:SEQ, mine] = part[0:SEQ, mine] + upper[...].astype(F32)
    keep[:, HALF:D] = part[:, half]
    away[:, HALF:D] = part[:, rest].astype(BF)


def before_kernel(
    at, done, theirs, gain, mark,
    given_out, back_in, normed_out, spread_out, second_out, back_out, gain_out, keep, away, whole, turned,
):
    tensor, core = at[0], at[1]
    mine = columns(tensor * WIDTH, WIDTH)
    half = columns(core * HALF, HALF)
    rest = columns((1 - core) * HALF, HALF)
    real = at_rows() < SEQ

    def sorted_rows(values, first):
        turned[...] = values.T.astype(BF)
        for out, y in ((keep, at[3]), (away, 1 - at[3])):
            for to, (k, z) in enumerate((k, z) for k in STEPS for z in range(8)):
                row = (z * 8 + y * 4 + (at[2] + k) % 4) * 16
                out[first + to * 16 : first + (to + 1) * 16, :] = turned[pl.ds(pl.multiple_of(row, 16), 16), :]

    whole[:, half] = done[:, 0:HALF].astype(F32)
    whole[:, rest] = theirs[:, 0:HALF].astype(F32)
    second_out[...] = whole[0:SEQ, mine].astype(BF)
    normed, spread = normalize(jnp.where(real, whole[...], 0.0))
    normed_out[...] = normed
    spread_out[...] = spread
    given = (normed * gain[...]).astype(BF)
    given_out[...] = given
    sorted_rows(given.astype(F32), 0)
    whole[:, half] = done[:, HALF:D].astype(F32)
    whole[:, rest] = theirs[:, HALF:D].astype(F32)
    back_out[...] = whole[0:SEQ, mine].astype(BF)
    gain_out[...] = whole[192:200, mine]
    back = jnp.where(real, whole[...], 0.0)
    back_in[...] = back.astype(BF)
    sorted_rows(back, 512)


def attention_kernel(at, given, back, qkv, proj, bias, gain_m, rows_out):
    rows = [dot(given[...], qkv[c]).astype(BF) for c in range(3)]
    grads = dot(back[...], proj[...]).astype(BF)
    valid = lax.broadcasted_iota(jnp.int32, (1, ROWS), 1) < SEQ
    query_parts, key_parts, value_parts, out_parts = [], [], [], []
    for h in range(4):
        s = slice(h * HEAD_DIM, (h + 1) * HEAD_DIM)
        q, k, v = (r[:, s] for r in rows)
        g = grads[:, s]
        scores = jnp.where(valid, dot_t(q, k) * FACTOR, -1e30)
        raised = jnp.exp(scores - jnp.max(scores, -1, keepdims=True))
        probs = raised / jnp.sum(raised, -1, keepdims=True)
        low = probs.astype(BF)
        out_parts.append(dot(low, v))
        grad_probs = dot_t(g, v)
        value_parts.append(t_dot(low, g))
        row_dot = jnp.sum(grad_probs * probs, -1, keepdims=True)
        grad_scores = (probs * (grad_probs - row_dot)).astype(BF)
        query_parts.append(dot(grad_scores, k) * FACTOR)
        key_parts.append(t_dot(grad_scores, q) * FACTOR)
    for n, parts in enumerate((query_parts, key_parts, value_parts, out_parts)):
        to = slice(n * WIDTH, (n + 1) * WIDTH)
        values = jnp.where(at_rows() == SEQ, bias[:, to], jnp.concatenate(parts, 1))
        if n == 0:
            values = jnp.where(at_rows() == SEQ + 1, gain_m[5:6, :], values)
        rows_out[:, to] = values.astype(BF)


def close_kernel(at, rows, normed, spread, gain, qkv, proj, keep, away, gain_out, part):
    core = at[1]

    def quarters(first_column):
        for k in range(2):
            to = slice(first_column + k * WIDTH, first_column + (k + 1) * WIDTH)
            keep[:, to] = part[:, columns((2 * k + core) * WIDTH, WIDTH)]
            away[:, to] = part[:, columns((2 * k + 1 - core) * WIDTH, WIDTH)].astype(BF)

    grad_norm = sum(dot_t(rows[:, c * WIDTH : (c + 1) * WIDTH], qkv[c]) for c in range(3))
    gain_part = jnp.sum(grad_norm * normed[...], 0, keepdims=True)
    for k in range(8):
        gain_out[k : k + 1, :] = gain_part[:, k * 128 : (k + 1) * 128]
    part[...] = norm_back(grad_norm, normed[...], spread[...], gain[...])
    quarters(HALF)
    part[...] = dot_t(rows[:, 3 * WIDTH :], proj[...])
    quarters(0)


def close_pair_kernel(at, keep, came, mine, sent):
    yhi = at[0] // 2
    for k in range(2):
        to = slice(k * WIDTH, (k + 1) * WIDTH)
        low, high = (
            keep[:, c : c + WIDTH] + came[:, c : c + WIDTH].astype(F32)
            for c in (k * HALF, k * HALF + WIDTH)
        )
        mine[:, to] = jnp.where(yhi == 0, low, high)
        sent[:, to] = jnp.where(yhi == 0, high, low).astype(BF)


def close_end_kernel(at, mine, came, first, lower, input_first, back_second):
    total = mine[...] + came[...].astype(F32)
    input_first[...] = (first[...].astype(F32) - total[0:SEQ, :WIDTH]).astype(BF)
    back_second[...] = (lower[...].astype(F32) + total[0:SEQ, WIDTH:]).astype(BF)


def over_z_each(values):
    for step in (4, 2, 1):
        values = values + lax.ppermute(values, "z", [(k, k ^ step) for k in range(8)])
    return values


def turn(left, turned):
    turned[...] = left[...].astype(F32).T.astype(BF)


def rows_of(turned, chosen, blocks):
    for to, b in enumerate(blocks):
        chosen[to * 16 : (to + 1) * 16, :] = turned[pl.ds(pl.multiple_of(b * 16, 16), 16), :]
    return chosen[...]


def far_kernel(at, left_in, left_out, right, far_a, far_b, turned_in, turned_out, chosen):
    turn(left_in, turned_in)
    turn(left_out, turned_out)
    blocks = [b * 4 + (at[2] + 2) % 4 for b in range(16)]
    far_a[...] = dot(rows_of(turned_in, chosen, blocks), right[:, :D]).astype(BF)
    far_b[...] = dot(rows_of(turned_out, chosen, blocks), right[:, D:]).astype(BF)


def near_kernel(at, turned_in, turned_out, right, a1, b1, a3, b3, a0, b0, chosen):
    for k, a, b in ((1, a1, b1), (3, a3, b3), (0, a0, b0)):
        blocks = [r * 4 + (at[2] + k) % 4 for r in range(16)]
        a[...] = dot(rows_of(turned_in, chosen, blocks), right[:, :D]).astype(BF)
        b[...] = dot(rows_of(turned_out, chosen, blocks), right[:, D:]).astype(BF)


def pieces_kernel(at, own_left, came_left, own_right, came_right, gain_a, *pieces):
    tail = own_right[192:ROWS, :].astype(F32) + came_right[192:ROWS, :].astype(F32)
    line = jnp.concatenate([gain_a[k : k + 1, :] for k in range(8)], 1)
    low = jnp.concatenate([tail[5:6], tail[6:7], line, jnp.zeros((5, D), F32)], 0).astype(BF)
    for to, piece in enumerate(pieces):
        for first, start, stop in ((0, 0, 3 * WIDTH), (512, 3 * WIDTH, D)):
            r = slice(first + to * 128, first + (to + 1) * 128)
            piece[0:128, start:stop] = (
                dot(own_left[r, :], own_right[:, start:stop]) + dot(came_left[r, :], came_right[:, start:stop])
            ).astype(BF)
        piece[128:136, :] = low


def added(a, b):
    return (a.astype(F32) + b.astype(F32)).astype(BF)


def sum_kernel(at, a0, a1, a2, b0, b1, b2, keep, away):
    split = a0.shape[1]
    for cols, terms in ((slice(0, split), (a0, a1, a2)), (slice(split, WIDE), (b0, b1, b2))):
        total = sum(t[...].astype(F32) for t in terms[1:]) + terms[0][...].astype(F32)
        for z in range(8):
            to = slice(z * 16, (z + 1) * 16)
            low, high = total[z * 32 : z * 32 + 16], total[z * 32 + 16 : z * 32 + 32]
            keep[to, cols] = jnp.where(at[3] == 0, low, high).astype(BF)
            away[to, cols] = jnp.where(at[3] == 0, high, low).astype(BF)


def merge_kernel(at, keep, came, a, b, c, d, total, gain_a):
    total[:, :WIDE] = (keep[...].astype(F32) + came[...].astype(F32)).astype(BF)
    terms = [r[...].astype(F32) for r in (a, b, c, d)]
    x_sum = terms[0] + terms[1] + terms[2] + terms[3]
    total[:, WIDE : WIDE + D] = x_sum[:128].astype(BF)
    low = x_sum[128:136]
    block = jnp.concatenate(
        [low[0:1, k * 128 : (k + 1) * 128] for k in range(8)]
        + [low[1:2, k * 128 : (k + 1) * 128] for k in range(2)]
        + [jnp.zeros((6, 128), F32)],
        0,
    ).astype(BF)
    total[:, WIDE + D :] = jnp.concatenate([block] * 8, 0)
    for k in range(8):
        gain_a[k : k + 1, :] = low[2:3, k * 128 : (k + 1) * 128]


def end_kernel(at, came, whole, inner, outer, bias, qkv, proj, gain_a, gain_m):
    total = came[0].astype(F32)
    for k in range(1, 8):
        total = total + came[k].astype(F32)
    inner[...] = total[:, :D]
    outer[...] = total[:, D:WIDE]
    for c in range(3):
        qkv[c] = total[:, WIDE + c * WIDTH : WIDE + (c + 1) * WIDTH]
    proj[...] = total[:, WIDE + 3 * WIDTH : WIDE + D]
    small = total[:, WIDE + D :]
    for k in range(8):
        bias[:, k * 128 : (k + 1) * 128] = small[k : k + 1, :]
    for k in range(2):
        to = slice(k * 128, (k + 1) * 128)
        gain_a[:, to] = sum(jnp.where(at[0] == t, whole[2 * t + k : 2 * t + k + 1, :], 0.0) for t in range(4))
        gain_m[:, to] = small[8 + k : 9 + k, :]


def on_device(
    out_first,
    out_second,
    grad_first,
    grad_second,
    gain_attn,
    gain_mlp,
    qkv_weight,
    proj_weight,
    inner_weight,
    inner_bias,
    outer_weight,
):
    yhi, core, ylo, x = (lax.axis_index(a) for a in ("yhi", "core", "ylo", "x"))
    at = jnp.stack([yhi * 2 + core, core, x, ylo]).astype(jnp.int32)
    first, second, upper, lower = (
        a.reshape(SEQ, WIDTH) for a in (out_first, out_second, grad_first, grad_second)
    )
    block = (ROWS, D)

    first_y, lower_y = swap(first, "yhi"), swap(lower, "yhi")
    first_c, lower_c = swap(first, "core"), swap(lower, "core")
    first_b, lower_b = swap(first_y, "core"), swap(lower_y, "core")
    gain_a = gain_attn.reshape(1, D)
    qkv = jnp.moveaxis(qkv_weight, 1, 0)
    proj = proj_weight
    keep, away, left_in, left_out, right, bias_part = call(
        mlp_kernel,
        [(block, F32), (block, BF), (block, BF), (block, BF), ((ROWS, 2 * D), BF), ((1, D), F32)],
        [pltpu.VMEM(block, F32), pltpu.VMEM(block, F32)],
        8 * ROWS * D * D,
        at,
        first,
        first_c,
        first_y,
        first_b,
        lower,
        lower_c,
        lower_y,
        lower_b,
        second,
        upper,
        passed(jnp.stack([gain_mlp, inner_bias]), outer_weight),
        inner_weight,
        outer_weight,
        pause(8 << 30),
    )
    come = swap(away, "core")
    pair = (keep + come.astype(F32)).astype(BF)
    other = swap(pair, "yhi")
    done = added(pair, other)
    theirs = swap(done, "core")

    far_a, far_b, turned_in, turned_out = call(
        far_kernel,
        [((256, D), BF), ((256, D), BF), ((D, ROWS), BF), ((D, ROWS), BF)],
        [pltpu.VMEM((256, ROWS), BF)],
        D * ROWS * D,
        at,
        left_in,
        left_out,
        right,
    )
    came_a, came_b = around(far_a, 1), around(far_b, -1)
    a1, b1, a3, b3, a0, b0 = call(
        near_kernel,
        [((256, D), BF)] * 6,
        [pltpu.VMEM((256, ROWS), BF)],
        3 * D * ROWS * D,
        at,
        turned_in,
        turned_out,
        right,
    )
    near_b, near_a = around(b1, 1), around(a3, -1)
    join_a, join_b = added(a1, came_a), added(b3, came_b)
    joined_a, joined_b = around(join_a, 1), around(join_b, -1)
    mlp_keep, mlp_away = call(
        sum_kernel,
        [((128, WIDE), BF)] * 2,
        [],
        1 << 24,
        at,
        a0,
        near_a,
        joined_a,
        b0,
        near_b,
        joined_b,
    )
    mlp_came = swap(mlp_away, "ylo")

    given, back, normed, spread, input_second, back_first, gain_rows, own_left, away_left = call(
        before_kernel,
        [
            (block, BF),
            (block, BF),
            (block, F32),
            ((ROWS, 1), F32),
            ((SEQ, WIDTH), BF),
            ((SEQ, WIDTH), BF),
            ((8, WIDTH), F32),
            ((D, ROWS), BF),
            ((D, ROWS), BF),
        ],
        [pltpu.VMEM(block, F32), pltpu.VMEM((D, ROWS), BF)],
        ROWS * D * D,
        at,
        done,
        theirs,
        gain_a,
        pause(1 << 20),
    )
    came_left = swap(away_left, "ylo")
    (rows,) = call(attention_kernel, [(block, BF)], [], 4 * ROWS * D * D, at, given, back, qkv, proj, bias_part, gain_rows)
    came_rows = swap(rows, "ylo")
    keep, away, gain_part = call(
        close_kernel,
        [(block, F32), (block, BF), ((8, 128), F32)],
        [pltpu.VMEM(block, F32)],
        2 * ROWS * D * D,
        at,
        rows,
        normed,
        spread,
        gain_a,
        qkv,
        proj,
    )
    pieces = call(
        pieces_kernel,
        [((136, D), BF)] * 4,
        [],
        2 * D * ROWS * D,
        at,
        own_left,
        came_left,
        rows,
        came_rows,
        over_z_each(gain_part),
    )
    came = [around(pieces[to], k) for to, k in enumerate(STEPS[:3])]
    mine, sent = call(
        close_pair_kernel,
        [((ROWS, HALF), F32), ((ROWS, HALF), BF)],
        [],
        1 << 22,
        at,
        keep,
        swap(away, "core"),
    )
    input_first, back_second = call(
        close_end_kernel,
        [((SEQ, WIDTH), BF), ((SEQ, WIDTH), BF)],
        [],
        1 << 22,
        at,
        mine,
        swap(sent, "yhi"),
        first,
        lower,
    )
    total, whole = call(
        merge_kernel,
        [((128, WIDE + D + 128), BF), ((8, 128), F32)],
        [],
        1 << 22,
        at,
        mlp_keep,
        mlp_came,
        pieces[3],
        *came,
    )
    for axis in ("core", "yhi", "ylo"):
        whole = whole + swap(whole, axis)
    came = lax.all_to_all(total.reshape(8, 16, -1), "z", 0, 0, tiled=True)
    grad_inner, grad_outer, bias_sum, grad_qkv, grad_proj, gain_a_sum, gain_m_sum = call(
        end_kernel,
        [
            ((16, D), F32),
            ((16, D), F32),
            ((1, D), F32),
            ((3, 16, WIDTH), F32),
            ((16, WIDTH), F32),
            ((1, WIDTH), F32),
            ((1, WIDTH), F32),
        ],
        [],
        1 << 20,
        at,
        came,
        whole,
    )

    shape_out = (1, SEQ, WIDTH)
    return (
        input_first.reshape(shape_out),
        input_second.reshape(shape_out),
        back_first.reshape(shape_out),
        back_second.reshape(shape_out),
        jnp.moveaxis(grad_qkv, 0, 1),
        grad_proj,
        grad_inner,
        bias_sum.reshape(D),
        grad_outer,
        gain_a_sum.reshape(WIDTH),
        gain_m_sum.reshape(WIDTH),
    )


def solution(mesh):
    split = Mesh(mesh.devices.reshape(8, 2, 4, 2, 2), AXES)
    rows = P(DP, None, TENSOR)
    return jax.shard_map(
        on_device,
        mesh=split,
        in_specs=(
            rows,
            rows,
            rows,
            rows,
            P(),
            P(),
            P(None, None, TENSOR),
            P(None, TENSOR),
            P(None, TENSOR),
            P(TENSOR),
            P(None, TENSOR),
        ),
        out_specs=(
            rows,
            rows,
            rows,
            rows,
            rows,
            P(DP, TENSOR),
            P(DP, TENSOR),
            P(TENSOR),
            P(DP, TENSOR),
            P(TENSOR),
            P(TENSOR),
        ),
        check_vma=False,
    )
```

```python
import jax
import jax.numpy as jnp
from jax import lax
from jax.experimental import pallas as pl
from jax.experimental.pallas import tpu as pltpu
from jax.sharding import Mesh
from jax.sharding import PartitionSpec as P

D = 1024
AXES = ("z", "ylo", "x", "yhi", "core")
DP = ("z", "ylo", "x")
TENSOR = ("yhi", "core")
SWAP = [(0, 1), (1, 0)]
BF = jnp.bfloat16
F32 = jnp.float32
SEQ = 197
ROWS = 208
WIDTH = 256
HALF = 512
WIDE = 2 * D
STEPS = (2, 1, 3, 0)
HEAD_DIM = 64
FACTOR = HEAD_DIM ** (-0.5)

epsilon = 1e-06


def swap(x, axis):
    return lax.ppermute(x, axis, SWAP)


def around(x, step):
    return lax.ppermute(x, "x", [(i, (i + step) % 4) for i in range(4)])


def normalize(values):
    centre = values - jnp.mean(values, -1, keepdims=True)
    spread = lax.rsqrt(jnp.mean(centre * centre, -1, keepdims=True) + epsilon)
    return (centre * spread, spread)


def norm_back(grad_in, normed, spread, gain):
    scaled = grad_in * gain
    first_mean = jnp.mean(scaled, -1, keepdims=True)
    second_mean = jnp.mean(scaled * normed, -1, keepdims=True)
    return spread * (scaled - first_mean - normed * second_mean)


def dot(a, b):
    return jnp.dot(a, b, preferred_element_type=F32)


def dot_t(a, b):
    return lax.dot_general(a, b, (((1,), (1,)), ((), ())), preferred_element_type=F32)


def t_dot(a, b):
    return lax.dot_general(a, b, (((0,), (0,)), ((), ())), preferred_element_type=F32)


def gelu_both(h):
    c = (2.0 / jnp.pi) ** 0.5
    square = h * h
    bent = jnp.tanh(c * h * (1.0 + 0.044715 * square))
    half = 0.5 * (1.0 + bent)
    slope = half + 0.5 * h * (1.0 - bent * bent) * (c * (1.0 + 3.0 * 0.044715 * square))
    return h * half, slope


def at_rows():
    return lax.broadcasted_iota(jnp.int32, (ROWS, 1), 0)


def columns(start, width):
    return pl.ds(pl.multiple_of(start, 128), width)


VMEM = pl.BlockSpec(memory_space=pltpu.VMEM)
SMEM = pl.BlockSpec(memory_space=pltpu.SMEM)
ANY = pl.BlockSpec(memory_space=pl.ANY)


def call(kernel, outs, scratch, flops, *args, limit=20):
    return pl.pallas_call(
        kernel,
        out_shape=[jax.ShapeDtypeStruct(s, d) for s, d in outs],
        in_specs=[SMEM] + [VMEM] * (len(args) - 1),
        out_specs=[VMEM] * len(outs),
        scratch_shapes=scratch,
        cost_estimate=pl.CostEstimate(flops=flops, bytes_accessed=4 << 20, transcendentals=0),
        compiler_params=pltpu.CompilerParams(vmem_limit_bytes=limit << 20),
    )(*args)


def pause_kernel(out):
    out[...] = jnp.zeros((8, 128), F32)


def pause(size):
    return pl.pallas_call(
        pause_kernel,
        out_shape=jax.ShapeDtypeStruct((8, 128), F32),
        out_specs=VMEM,
        cost_estimate=pl.CostEstimate(flops=size, bytes_accessed=size >> 13, transcendentals=0),
        compiler_params=pltpu.CompilerParams(vmem_limit_bytes=1 << 20),
    )()


def pass_kernel(values, weight, out):
    out[...] = values[...]


def passed(values, weight):
    return pl.pallas_call(
        pass_kernel,
        out_shape=jax.ShapeDtypeStruct(values.shape, values.dtype),
        in_specs=[VMEM, ANY],
        out_specs=VMEM,
        cost_estimate=pl.CostEstimate(flops=8 << 30, bytes_accessed=1 << 20, transcendentals=0),
        compiler_params=pltpu.CompilerParams(vmem_limit_bytes=1 << 20),
    )(values, weight)


def mlp_kernel(
    at, f0, f1, f2, f3, l0, l1, l2, l3, second, upper, vectors, inner, outer, mark,
    keep, away, left_in, left_out, right, bias_part, whole, part,
):
    tensor, core = at[0], at[1]
    half = columns(core * HALF, HALF)
    rest = columns((1 - core) * HALF, HALF)
    gain, bias = vectors[0:1, :], vectors[1:2, :]

    def gathered(blocks):
        whole[192:ROWS, :] = jnp.zeros((ROWS - 192, D), F32)
        for k, b in enumerate(blocks):
            whole[0:SEQ, columns((tensor ^ k) * WIDTH, WIDTH)] = b[...].astype(F32)
        return whole[...]

    normed, spread = normalize(gathered((f0, f1, f2, f3)))
    given = (normed * gain).astype(BF)
    left_in[...] = given
    hidden = dot(given, inner[...]) + bias
    active, slope = gelu_both(hidden)
    active = active.astype(BF)
    right[:, D:] = active
    part[...] = -dot_t(active, outer[...])
    mine = columns(tensor * WIDTH, WIDTH)
    part[0:SEQ, mine] = part[0:SEQ, mine] + second[...].astype(F32)
    keep[:, 0:HALF] = part[:, half]
    away[:, 0:HALF] = part[:, rest].astype(BF)

    lower = gathered((l0, l1, l2, l3)).astype(BF)
    left_out[...] = lower
    grad_hidden = (dot(lower, outer[...]) * slope).astype(BF)
    right[:, :D] = grad_hidden
    bias_part[...] = jnp.sum(grad_hidden.astype(F32), 0, keepdims=True)
    grad_norm = dot_t(grad_hidden, inner[...])
    gain_part = jnp.sum(grad_norm * normed, 0, keepdims=True)
    back = norm_back(grad_norm, normed, spread, gain)
    part[...] = jnp.where(at_rows() == SEQ, gain_part, back)
    part[0:SEQ, mine] = part[0:SEQ, mine] + upper[...].astype(F32)
    keep[:, HALF:D] = part[:, half]
    away[:, HALF:D] = part[:, rest].astype(BF)


def before_kernel(
    at, done, theirs, gain, mark,
    given_out, back_in, normed_out, spread_out, second_out, back_out, gain_out, keep, away, whole, turned,
):
    tensor, core = at[0], at[1]
    mine = columns(tensor * WIDTH, WIDTH)
    half = columns(core * HALF, HALF)
    rest = columns((1 - core) * HALF, HALF)
    real = at_rows() < SEQ

    def sorted_rows(values, first):
        turned[...] = values.T.astype(BF)
        for out, y in ((keep, at[3]), (away, 1 - at[3])):
            for to, (k, z) in enumerate((k, z) for k in STEPS for z in range(8)):
                row = (z * 8 + y * 4 + (at[2] + k) % 4) * 16
                out[first + to * 16 : first + (to + 1) * 16, :] = turned[pl.ds(pl.multiple_of(row, 16), 16), :]

    whole[:, half] = done[:, 0:HALF].astype(F32)
    whole[:, rest] = theirs[:, 0:HALF].astype(F32)
    second_out[...] = whole[0:SEQ, mine].astype(BF)
    normed, spread = normalize(jnp.where(real, whole[...], 0.0))
    normed_out[...] = normed
    spread_out[...] = spread
    given = (normed * gain[...]).astype(BF)
    given_out[...] = given
    sorted_rows(given.astype(F32), 0)
    whole[:, half] = done[:, HALF:D].astype(F32)
    whole[:, rest] = theirs[:, HALF:D].astype(F32)
    back_out[...] = whole[0:SEQ, mine].astype(BF)
    gain_out[...] = whole[192:200, mine]
    back = jnp.where(real, whole[...], 0.0)
    back_in[...] = back.astype(BF)
    sorted_rows(back, 512)


def attention_kernel(at, given, back, qkv, proj, bias, gain_m, rows_out):
    rows = [dot(given[...], qkv[c]).astype(BF) for c in range(3)]
    grads = dot(back[...], proj[...]).astype(BF)
    valid = lax.broadcasted_iota(jnp.int32, (1, ROWS), 1) < SEQ
    query_parts, key_parts, value_parts, out_parts = [], [], [], []
    for h in range(4):
        s = slice(h * HEAD_DIM, (h + 1) * HEAD_DIM)
        q, k, v = (r[:, s] for r in rows)
        g = grads[:, s]
        scores = jnp.where(valid, dot_t(q, k) * FACTOR, -1e30)
        raised = jnp.exp(scores - jnp.max(scores, -1, keepdims=True))
        probs = raised / jnp.sum(raised, -1, keepdims=True)
        low = probs.astype(BF)
        out_parts.append(dot(low, v))
        grad_probs = dot_t(g, v)
        value_parts.append(t_dot(low, g))
        row_dot = jnp.sum(grad_probs * probs, -1, keepdims=True)
        grad_scores = (probs * (grad_probs - row_dot)).astype(BF)
        query_parts.append(dot(grad_scores, k) * FACTOR)
        key_parts.append(t_dot(grad_scores, q) * FACTOR)
    for n, parts in enumerate((query_parts, key_parts, value_parts, out_parts)):
        to = slice(n * WIDTH, (n + 1) * WIDTH)
        values = jnp.where(at_rows() == SEQ, bias[:, to], jnp.concatenate(parts, 1))
        if n == 0:
            values = jnp.where(at_rows() == SEQ + 1, gain_m[5:6, :], values)
        rows_out[:, to] = values.astype(BF)


def close_kernel(at, rows, normed, spread, gain, qkv, proj, keep, away, gain_out, part):
    core = at[1]

    def quarters(first_column):
        for k in range(2):
            to = slice(first_column + k * WIDTH, first_column + (k + 1) * WIDTH)
            keep[:, to] = part[:, columns((2 * k + core) * WIDTH, WIDTH)]
            away[:, to] = part[:, columns((2 * k + 1 - core) * WIDTH, WIDTH)].astype(BF)

    grad_norm = sum(dot_t(rows[:, c * WIDTH : (c + 1) * WIDTH], qkv[c]) for c in range(3))
    gain_part = jnp.sum(grad_norm * normed[...], 0, keepdims=True)
    for k in range(8):
        gain_out[k : k + 1, :] = gain_part[:, k * 128 : (k + 1) * 128]
    part[...] = norm_back(grad_norm, normed[...], spread[...], gain[...])
    quarters(HALF)
    part[...] = dot_t(rows[:, 3 * WIDTH :], proj[...])
    quarters(0)


def close_pair_kernel(at, keep, came, mine, sent):
    yhi = at[0] // 2
    for k in range(2):
        to = slice(k * WIDTH, (k + 1) * WIDTH)
        low, high = (
            keep[:, c : c + WIDTH] + came[:, c : c + WIDTH].astype(F32)
            for c in (k * HALF, k * HALF + WIDTH)
        )
        mine[:, to] = jnp.where(yhi == 0, low, high)
        sent[:, to] = jnp.where(yhi == 0, high, low).astype(BF)


def close_end_kernel(at, mine, came, first, lower, input_first, back_second):
    total = mine[...] + came[...].astype(F32)
    input_first[...] = (first[...].astype(F32) - total[0:SEQ, :WIDTH]).astype(BF)
    back_second[...] = (lower[...].astype(F32) + total[0:SEQ, WIDTH:]).astype(BF)


def over_z_each(values):
    for step in (4, 2, 1):
        values = values + lax.ppermute(values, "z", [(k, k ^ step) for k in range(8)])
    return values


def turn(left, turned):
    turned[...] = left[...].astype(F32).T.astype(BF)


def rows_of(turned, chosen, blocks):
    for to, b in enumerate(blocks):
        chosen[to * 16 : (to + 1) * 16, :] = turned[pl.ds(pl.multiple_of(b * 16, 16), 16), :]
    return chosen[...]


def far_kernel(at, left_in, left_out, right, far_a, far_b, turned_in, turned_out, chosen):
    turn(left_in, turned_in)
    turn(left_out, turned_out)
    blocks = [b * 4 + (at[2] + 2) % 4 for b in range(16)]
    far_a[...] = dot(rows_of(turned_in, chosen, blocks), right[:, :D]).astype(BF)
    far_b[...] = dot(rows_of(turned_out, chosen, blocks), right[:, D:]).astype(BF)


def near_kernel(at, turned_in, turned_out, right, a1, b1, a3, b3, a0, b0, chosen):
    for k, a, b in ((1, a1, b1), (3, a3, b3), (0, a0, b0)):
        blocks = [r * 4 + (at[2] + k) % 4 for r in range(16)]
        a[...] = dot(rows_of(turned_in, chosen, blocks), right[:, :D]).astype(BF)
        b[...] = dot(rows_of(turned_out, chosen, blocks), right[:, D:]).astype(BF)


def pieces_kernel(start, at, own_left, came_left, own_right, came_right, gain_a, *pieces):
    tail = own_right[192:ROWS, :].astype(F32) + came_right[192:ROWS, :].astype(F32)
    line = jnp.concatenate([gain_a[k : k + 1, :] for k in range(8)], 1)
    low = jnp.concatenate([tail[5:6], tail[6:7], line, jnp.zeros((5, D), F32)], 0).astype(BF)
    for to, piece in enumerate(pieces, start):
        for first, low_c, stop in ((0, 0, 3 * WIDTH), (512, 3 * WIDTH, D)):
            r = slice(first + to * 128, first + (to + 1) * 128)
            piece[0:128, low_c:stop] = (
                dot(own_left[r, :], own_right[:, low_c:stop]) + dot(came_left[r, :], came_right[:, low_c:stop])
            ).astype(BF)
        piece[128:136, :] = low


def added(a, b):
    return (a.astype(F32) + b.astype(F32)).astype(BF)


def sum_kernel(at, a0, a1, a2, b0, b1, b2, keep, away):
    split = a0.shape[1]
    for cols, terms in ((slice(0, split), (a0, a1, a2)), (slice(split, WIDE), (b0, b1, b2))):
        total = sum(t[...].astype(F32) for t in terms[1:]) + terms[0][...].astype(F32)
        for z in range(8):
            to = slice(z * 16, (z + 1) * 16)
            low, high = total[z * 32 : z * 32 + 16], total[z * 32 + 16 : z * 32 + 32]
            keep[to, cols] = jnp.where(at[3] == 0, low, high).astype(BF)
            away[to, cols] = jnp.where(at[3] == 0, high, low).astype(BF)


def merge_kernel(at, keep, came, a, b, c, d, total, gain_a):
    total[:, :WIDE] = (keep[...].astype(F32) + came[...].astype(F32)).astype(BF)
    terms = [r[...].astype(F32) for r in (a, b, c, d)]
    x_sum = terms[0] + terms[1] + terms[2] + terms[3]
    total[:, WIDE : WIDE + D] = x_sum[:128].astype(BF)
    low = x_sum[128:136]
    block = jnp.concatenate(
        [low[0:1, k * 128 : (k + 1) * 128] for k in range(8)]
        + [low[1:2, k * 128 : (k + 1) * 128] for k in range(2)]
        + [jnp.zeros((6, 128), F32)],
        0,
    ).astype(BF)
    total[:, WIDE + D :] = jnp.concatenate([block] * 8, 0)
    for k in range(8):
        gain_a[k : k + 1, :] = low[2:3, k * 128 : (k + 1) * 128]


def end_kernel(at, came, whole, inner, outer, bias, qkv, proj, gain_a, gain_m):
    total = came[0].astype(F32)
    for k in range(1, 8):
        total = total + came[k].astype(F32)
    inner[...] = total[:, :D]
    outer[...] = total[:, D:WIDE]
    for c in range(3):
        qkv[c] = total[:, WIDE + c * WIDTH : WIDE + (c + 1) * WIDTH]
    proj[...] = total[:, WIDE + 3 * WIDTH : WIDE + D]
    small = total[:, WIDE + D :]
    for k in range(8):
        bias[:, k * 128 : (k + 1) * 128] = small[k : k + 1, :]
    for k in range(2):
        to = slice(k * 128, (k + 1) * 128)
        gain_a[:, to] = sum(jnp.where(at[0] == t, whole[2 * t + k : 2 * t + k + 1, :], 0.0) for t in range(4))
        gain_m[:, to] = small[8 + k : 9 + k, :]


def on_device(
    out_first,
    out_second,
    grad_first,
    grad_second,
    gain_attn,
    gain_mlp,
    qkv_weight,
    proj_weight,
    inner_weight,
    inner_bias,
    outer_weight,
):
    yhi, core, ylo, x = (lax.axis_index(a) for a in ("yhi", "core", "ylo", "x"))
    at = jnp.stack([yhi * 2 + core, core, x, ylo]).astype(jnp.int32)
    first, second, upper, lower = (
        a.reshape(SEQ, WIDTH) for a in (out_first, out_second, grad_first, grad_second)
    )
    block = (ROWS, D)

    first_y, lower_y = swap(first, "yhi"), swap(lower, "yhi")
    first_c, lower_c = swap(first, "core"), swap(lower, "core")
    first_b, lower_b = swap(first_y, "core"), swap(lower_y, "core")
    gain_a = gain_attn.reshape(1, D)
    qkv = jnp.moveaxis(qkv_weight, 1, 0)
    proj = proj_weight
    keep, away, left_in, left_out, right, bias_part = call(
        mlp_kernel,
        [(block, F32), (block, BF), (block, BF), (block, BF), ((ROWS, 2 * D), BF), ((1, D), F32)],
        [pltpu.VMEM(block, F32), pltpu.VMEM(block, F32)],
        8 * ROWS * D * D,
        at,
        first,
        first_c,
        first_y,
        first_b,
        lower,
        lower_c,
        lower_y,
        lower_b,
        second,
        upper,
        passed(jnp.stack([gain_mlp, inner_bias]), outer_weight),
        inner_weight,
        outer_weight,
        pause(8 << 30),
    )
    come = swap(away, "core")
    pair = (keep + come.astype(F32)).astype(BF)
    other = swap(pair, "yhi")
    done = added(pair, other)
    theirs = swap(done, "core")

    far_a, far_b, turned_in, turned_out = call(
        far_kernel,
        [((256, D), BF), ((256, D), BF), ((D, ROWS), BF), ((D, ROWS), BF)],
        [pltpu.VMEM((256, ROWS), BF)],
        D * ROWS * D,
        at,
        left_in,
        left_out,
        right,
    )
    came_a, came_b = around(far_a, 1), around(far_b, -1)
    a1, b1, a3, b3, a0, b0 = call(
        near_kernel,
        [((256, D), BF)] * 6,
        [pltpu.VMEM((256, ROWS), BF)],
        3 * D * ROWS * D,
        at,
        turned_in,
        turned_out,
        right,
    )
    near_b, near_a = around(b1, 1), around(a3, -1)
    join_a, join_b = added(a1, came_a), added(b3, came_b)
    joined_a, joined_b = around(join_a, 1), around(join_b, -1)
    mlp_keep, mlp_away = call(
        sum_kernel,
        [((128, WIDE), BF)] * 2,
        [],
        1 << 24,
        at,
        a0,
        near_a,
        joined_a,
        b0,
        near_b,
        joined_b,
    )
    mlp_came = swap(mlp_away, "ylo")

    given, back, normed, spread, input_second, back_first, gain_rows, own_left, away_left = call(
        before_kernel,
        [
            (block, BF),
            (block, BF),
            (block, F32),
            ((ROWS, 1), F32),
            ((SEQ, WIDTH), BF),
            ((SEQ, WIDTH), BF),
            ((8, WIDTH), F32),
            ((D, ROWS), BF),
            ((D, ROWS), BF),
        ],
        [pltpu.VMEM(block, F32), pltpu.VMEM((D, ROWS), BF)],
        ROWS * D * D,
        at,
        done,
        theirs,
        gain_a,
        pause(1 << 20),
    )
    came_left = swap(away_left, "ylo")
    (rows,) = call(attention_kernel, [(block, BF)], [], 4 * ROWS * D * D, at, given, back, qkv, proj, bias_part, gain_rows)
    came_rows = swap(rows, "ylo")
    keep, away, gain_part = call(
        close_kernel,
        [(block, F32), (block, BF), ((8, 128), F32)],
        [pltpu.VMEM(block, F32)],
        2 * ROWS * D * D,
        at,
        rows,
        normed,
        spread,
        gain_a,
        qkv,
        proj,
    )
    gain_z = over_z_each(gain_part)

    def some_pieces(start, count):
        def kernel(*refs):
            pieces_kernel(start, *refs)

        return call(
            kernel,
            [((136, D), BF)] * count,
            [],
            D * ROWS * D * count // 2,
            at,
            own_left,
            came_left,
            rows,
            came_rows,
            gain_z,
        )

    pieces = [*some_pieces(0, 1), *some_pieces(1, 3)]
    came = [around(pieces[to], k) for to, k in enumerate(STEPS[:3])]
    mine, sent = call(
        close_pair_kernel,
        [((ROWS, HALF), F32), ((ROWS, HALF), BF)],
        [],
        1 << 22,
        at,
        keep,
        swap(away, "core"),
    )
    input_first, back_second = call(
        close_end_kernel,
        [((SEQ, WIDTH), BF), ((SEQ, WIDTH), BF)],
        [],
        1 << 22,
        at,
        mine,
        swap(sent, "yhi"),
        first,
        lower,
    )
    total, whole = call(
        merge_kernel,
        [((128, WIDE + D + 128), BF), ((8, 128), F32)],
        [],
        1 << 22,
        at,
        mlp_keep,
        mlp_came,
        pieces[3],
        *came,
    )
    for axis in ("core", "yhi", "ylo"):
        whole = whole + swap(whole, axis)
    came = lax.all_to_all(total.reshape(8, 16, -1), "z", 0, 0, tiled=True)
    grad_inner, grad_outer, bias_sum, grad_qkv, grad_proj, gain_a_sum, gain_m_sum = call(
        end_kernel,
        [
            ((16, D), F32),
            ((16, D), F32),
            ((1, D), F32),
            ((3, 16, WIDTH), F32),
            ((16, WIDTH), F32),
            ((1, WIDTH), F32),
            ((1, WIDTH), F32),
        ],
        [],
        1 << 20,
        at,
        came,
        whole,
    )

    shape_out = (1, SEQ, WIDTH)
    return (
        input_first.reshape(shape_out),
        input_second.reshape(shape_out),
        back_first.reshape(shape_out),
        back_second.reshape(shape_out),
        jnp.moveaxis(grad_qkv, 0, 1),
        grad_proj,
        grad_inner,
        bias_sum.reshape(D),
        grad_outer,
        gain_a_sum.reshape(WIDTH),
        gain_m_sum.reshape(WIDTH),
    )


def solution(mesh):
    split = Mesh(mesh.devices.reshape(8, 2, 4, 2, 2), AXES)
    rows = P(DP, None, TENSOR)
    return jax.shard_map(
        on_device,
        mesh=split,
        in_specs=(
            rows,
            rows,
            rows,
            rows,
            P(),
            P(),
            P(None, None, TENSOR),
            P(None, TENSOR),
            P(None, TENSOR),
            P(TENSOR),
            P(None, TENSOR),
        ),
        out_specs=(
            rows,
            rows,
            rows,
            rows,
            rows,
            P(DP, TENSOR),
            P(DP, TENSOR),
            P(TENSOR),
            P(DP, TENSOR),
            P(TENSOR),
            P(TENSOR),
        ),
        check_vma=False,
    )
```
